32 devices in a mesh: parts: 2 (over x), expert: 16 (over z, y, core).
Axes of the slice: x: 2, y: 2, z: 4, core: 2. Of those that a mesh axis runs over, the one named last changes fastest.
Arguments:
- tokens: bfloat16 [2, 128, 7168], P(None, ('parts', 'expert')), parts along dimension 1, may hold values from -6 to 6
- live_rows: int32 [2, 32], P(None, ('parts', 'expert')), parts along dimension 1, may hold values from 3 to 4
- expert_ids: int32 [1, 2, 128, 8], P(None, None, ('parts', 'expert')), parts along dimension 2, may hold values from 0 to 15, all different within a row; in each aligned block of 4 rows (0 to 3, 4 to 7, ..., all dimensions but the last counted through in order) at most 2 rows name the same one
- gate_weights: float32 [1, 2, 128, 8], P(None, None, ('parts', 'expert')), parts along dimension 2, may hold values from 0.25 to 2.5
- norm_gain: float32 [1, 7168], replicated, may hold values from 0.1 to 1.9
- expert_gate_up: bfloat16 [1, 16, 7168, 2048], P(None, 'expert'), may hold values from -0.0625 to 0.0625
- expert_down: bfloat16 [1, 16, 1024, 7168], P(None, 'expert'), may hold values from -0.1875 to 0.1875
- shared_gate_up: bfloat16 [1, 7168, 2048], P(None, 'expert'), may hold values from -0.0625 to 0.0625
- shared_down: bfloat16 [1, 1024, 7168], P(None, None, 'expert'), may hold values from -0.1875 to 0.1875
Outputs:
- hidden_out: bfloat16 [2, 128, 7168], P(None, ('parts', 'expert')), parts along dimension 1
The draws below stay inside these ranges and needn't reach their ends.
There are 2 independent parts, one for each index of `parts`. The reference program is written for one: setup_inputs(seed, part) draws one part's arguments, and reference() takes and returns one part's arrays. A program takes and returns all parts, laid end to end along the dimension named above; an argument that names none is the same for every part. Nothing has to cross between parts.
Inputs may be any that keep to these rules, and one draw needn't show every extreme that they name: `expert_ids`: the 8 ids of a row differ; within the rows of one device for one layer and step, no expert is named by more than 2 rows, a bound that some block reaches.
All inputs are finite; a program needn't handle non-finite values.
Results may differ from the reference program's by a relative error of at most 0.0068.
Values may be sent and summed in bfloat16 or wider, within the bound.
A program may use at most 128 MiB of HBM per device.

```python
import math
import jax
import jax.numpy as jnp
import numpy as np
from jax import lax

D = 7168
TOP = 8
HID = 1024
SHARED = 1024
EXPERTS = 16
LAYERS = 1
STEPS = 2
ROWS_DEV = 4
GROUP = 1
TOKENS = 64
CAP = 2
N_EXPERT = 16


def with_ends(values, own_key, least, top_value):
    index_at = [jax.random.randint(jax.random.fold_in(own_key, axis), (), 0, length) for axis, length in enumerate(values.shape)]
    longest = values.shape.index(max(values.shape))
    beside = index_at[:longest] + [(index_at[longest] + 1) % values.shape[longest]] + index_at[longest + 1:]
    return values.at[tuple(index_at)].set(least).at[tuple(beside)].set(top_value)


def levels(own_key, shape, shards, low, top_value):
    gain, own = 1.0, jax.random.fold_in(own_key, 6)
    for axis_at, shards_of in shards:
        heights = jnp.exp(jax.random.uniform(jax.random.fold_in(own, axis_at), (shards_of,), jnp.float32, low / len(shards), top_value / len(shards)))
        gain = gain * jnp.repeat(heights, shape[axis_at] // shards_of).reshape([-1 if axis == axis_at else 1 for axis in range(len(shape))])
    return gain


def deal_out(stream_key, own, number, rows, number_of, top, most, lean):
    sequence = jax.random.permutation(stream_key, number_of)
    packed, common = shares(number_of, rows * top, most, lean, True), shares(number_of, rows * top, most, lean, False)
    places = jnp.arange(number_of)

    def named(sizes, rotation):
        used = int((sizes > 0).sum())
        fixed = max(1, used // 4)
        shifted = fixed + (places - fixed + rotation * (used - fixed)) % max(1, number_of - fixed)
        return jnp.zeros((number_of,), jnp.int32).at[sequence[jnp.where(places < fixed, places, shifted)]].set(jnp.asarray(sizes, jnp.int32))

    sizes = jnp.where(number % 4 == 0, named(packed, number // 4), named(common, number - number // 4 - 1))
    mixed = jax.random.permutation(jax.random.fold_in(own, 3), number_of)
    donor, taker = mixed[0:number_of // 2 * 2:2], mixed[1:number_of // 2 * 2:2]
    room = jnp.minimum(sizes[donor] - 1, most - sizes[taker]) // 2
    room = jnp.where((donor == sequence[0]) | (taker == sequence[0]) | (sizes[taker] == 0), 0, jnp.maximum(room, 0))
    shifted = jax.random.randint(jax.random.fold_in(own, 4), (number_of // 2,), 0, 1 << 20) % (room + 1)
    sizes = sizes.at[donor].add(-shifted).at[taker].add(shifted)
    items = jnp.searchsorted(jnp.cumsum(sizes), jnp.arange(rows * top), side="right").astype(jnp.int32)
    table = items.reshape(top, rows).T
    table = table[jax.random.permutation(jax.random.fold_in(own, 1), rows)]
    rotation = jax.random.randint(jax.random.fold_in(own, 2), (rows, 1), 0, top)
    return jnp.take_along_axis(table, (jnp.arange(top)[None, :] + rotation) % top, axis=1)


def shares(count, total, most, lean, full):
    loads = [(1 << 20) // math.isqrt(rank ** lean) + 1 for rank in range(1, count + 1)]
    largest = most if full else min(most, max(-(-total // count), total * loads[0] // sum(loads)))
    least = 1 if total - largest >= count - 1 else 0
    given, surplus = [largest] + [least] * (count - 1), total - largest - least * (count - 1)
    while surplus > 0:
        candidates = [i for i in range(1, count) if given[i] < largest] or [i for i in range(1, count) if given[i] < most]
        mass, left = sum([loads[i] for i in candidates]), surplus
        for i in candidates:
            more = min(most - given[i], max(1, left * loads[i] // mass), surplus)
            given[i] = given[i] + more
            surplus = surplus - more
    return np.array(given)


def centred(key, extent, spread, bound, shards=(), held_as=jnp.bfloat16):
    entries = spread * jax.random.normal(key, extent, jnp.float32)
    if shards:
        entries = entries * levels(key, extent, shards, -0.22, 0.18)
    return jnp.clip(entries, -bound, bound).astype(held_as)


def setup_inputs(seed: int = 0, part: int = 0) -> dict:
    arg_keys = jax.random.split(jax.random.key(seed), 10)
    part_splits = jax.random.split(jax.random.fold_in(arg_keys[9], part), 10)
    tokens = centred(part_splits[0], (STEPS, TOKENS, D), 1.0, 6.0, ((1, 16),))
    live_rows = with_ends(jax.random.randint(part_splits[1], (STEPS, N_EXPERT), (3 * ROWS_DEV) // 4, ROWS_DEV + 1), jax.random.fold_in(part_splits[1], 1), (3 * ROWS_DEV) // 4, ROWS_DEV).astype(jnp.int32)
    expert_ids_keys = jax.random.split(jax.random.fold_in(part_splits[2], 1), LAYERS * STEPS * TOKENS // ROWS_DEV)
    expert_ids_turns = jax.random.permutation(jax.random.fold_in(part_splits[2], 3), LAYERS * STEPS * TOKENS // ROWS_DEV)
    expert_ids = jax.vmap(lambda own, number: deal_out(jax.random.fold_in(part_splits[2], 2), own, number, ROWS_DEV, EXPERTS, TOP, CAP, 2))(expert_ids_keys, expert_ids_turns).reshape((LAYERS, STEPS, TOKENS, TOP))
    gate_weights = jnp.clip(jnp.exp(math.log(2.5) - 2.3025851 * jax.random.uniform(part_splits[3], (LAYERS, STEPS, TOKENS, TOP), jnp.float32) ** levels(part_splits[3], (LAYERS, STEPS, TOKENS, TOP), ((2, 16),), -0.2, 0.2)), 0.25, 2.5)
    norm_gain = jnp.clip(1.0 + 0.18 * jax.random.normal(arg_keys[4], (LAYERS, D), jnp.float32), 0.1, 1.9)
    expert_gate_up = centred(arg_keys[5], (LAYERS, EXPERTS * GROUP, D, 2 * HID // GROUP), D ** -0.5, 0.0625, ((1, 16),))
    expert_down = centred(arg_keys[6], (LAYERS, EXPERTS * GROUP, HID // GROUP, D), HID ** -0.5, 0.1875, ((1, 16),))
    shared_gate_up = centred(arg_keys[7], (LAYERS, D, 2 * SHARED), D ** -0.5, 0.0625, ((1, 16),))
    shared_down = centred(arg_keys[8], (LAYERS, SHARED, D), SHARED ** -0.5, 0.1875, ((2, 16),))
    return {"tokens": tokens, "live_rows": live_rows, "expert_ids": expert_ids, "gate_weights": gate_weights, "norm_gain": norm_gain, "expert_gate_up": expert_gate_up, "expert_down": expert_down, "shared_gate_up": shared_gate_up, "shared_down": shared_down}


EPSILON = 1e-06

def rms_normed(hidden, gain_row):
    widened = hidden.astype(jnp.float32)
    scaling = lax.rsqrt(lax.optimization_barrier(jnp.mean(widened * widened, axis=-1, keepdims=True)) + EPSILON)
    return (widened * scaling * gain_row).astype(jnp.bfloat16)

def swiglu(inputs, gate_up, down_proj, unit_count):
    projected = jnp.dot(inputs, gate_up, preferred_element_type=jnp.float32)
    activated = (jax.nn.silu(projected[:, :unit_count]) * projected[:, unit_count:]).astype(jnp.bfloat16)
    return jnp.dot(activated, down_proj, preferred_element_type=jnp.float32).astype(jnp.bfloat16)

def partial_swiglu(inputs, gate_up, down_proj, unit_count):
    projected = jnp.dot(inputs, gate_up, preferred_element_type=jnp.float32)
    activated = (jax.nn.silu(projected[:, :unit_count]) * projected[:, unit_count:]).astype(jnp.bfloat16)
    return jnp.dot(activated, down_proj, preferred_element_type=jnp.float32)

def routed_sum(normed, id_block, gate_block, is_live, gate_up, down_proj):
    unit_block = HID // GROUP
    grouped_up = gate_up.reshape(EXPERTS, GROUP, D, 2 * unit_block)
    grouped_down = down_proj.reshape(EXPERTS, GROUP, unit_block, D)
    flat_ids = jnp.where(is_live[:, None], id_block, -1).reshape(-1)
    flat_gates = gate_block.reshape(-1)
    slot_count = N_EXPERT * CAP

    def one_expert(carry_sum, expert):
        hit_mask = (flat_ids == expert).astype(jnp.int32)
        ordering = jnp.argsort(-hit_mask, stable=True)[:slot_count]
        picked = hit_mask[ordering].astype(jnp.float32)
        row_index = (ordering // TOP).astype(jnp.int32)
        chosen = normed[row_index]
        upper = grouped_up[expert]
        lower = grouped_down[expert]
        total = jnp.zeros((slot_count, D), jnp.float32)
        for member in range(GROUP):
            total = total + partial_swiglu(chosen, upper[member], lower[member], unit_block)
        outputs = total.astype(jnp.bfloat16)
        weighted = (flat_gates[ordering] * picked)[:, None] * outputs.astype(jnp.float32)
        return (carry_sum.at[row_index].add(weighted), None)
    start_sum = jnp.zeros((TOKENS, D), jnp.float32)
    final_sum, _ = lax.scan(one_expert, start_sum, jnp.arange(EXPERTS, dtype=jnp.int32))
    return final_sum

def reference(tokens, live_rows, expert_ids, gate_weights, norm_gain, expert_gate_up, expert_down, shared_gate_up, shared_down):
    position = jnp.arange(TOKENS, dtype=jnp.int32)
    results = []
    for step_at in range(STEPS):
        is_live = position % ROWS_DEV < jnp.repeat(live_rows[step_at], ROWS_DEV)
        hidden = tokens[step_at]
        for layer_at in range(LAYERS):
            normed = rms_normed(hidden, norm_gain[layer_at])
            combined = routed_sum(normed, expert_ids[layer_at, step_at], gate_weights[layer_at, step_at], is_live, expert_gate_up[layer_at], expert_down[layer_at])
            shared = swiglu(normed, shared_gate_up[layer_at], shared_down[layer_at], SHARED)
            combined = combined + shared.astype(jnp.float32)
            hidden = (hidden.astype(jnp.float32) + jnp.where(is_live[:, None], combined, 0.0)).astype(jnp.bfloat16)
        results.append(hidden)
    return jnp.stack(results)
```

```python
import functools

import jax
import jax.numpy as jnp
from jax import lax
from jax.experimental import pallas as pl
from jax.experimental.pallas import tpu as pltpu
from jax.sharding import PartitionSpec as P

EXPERTS = 16
EPSILON = 1e-06
LANES = 128
BF16 = jnp.bfloat16
F32 = jnp.float32


def dotted(left, right):
    return jnp.dot(left, right, preferred_element_type=F32)


def layer_kernel(
    n,
    experts,
    group,
    chunk,
    window,
    tokens_ref,
    live_ref,
    ids_ref,
    gates_ref,
    gain_ref,
    gate_up_hbm,
    down_hbm,
    shared_up_hbm,
    shared_down_hbm,
    routed_out,
    shared_out,
    own_n,
    peer_n,
    x_all,
    gate_up,
    down,
    shared_up,
    shared_down,
    hidden,
    sh_part,
    sh_send,
    sh_peer,
    sh_y,
    sh_yr,
    sh_z,
    sh_zr,
    sh_hidden,
    so_send,
    so_recv,
    so_f,
    so_fr,
    part,
    r_p,
    r_pr,
    r_y,
    r_yr,
    r_z,
    r_zr,
    keep,
    res,
    res_r,
    w_sem,
    n_sem,
    xz_s,
    xy_s,
    xp_s,
    x_r,
    hz_s,
    hy_s,
    hp_s,
    h_r,
    sp_sem,
    sy_sem,
    sz_s,
    sz_r,
    so_s,
    so_r,
    p_s,
    p_r,
    y_s,
    y_r,
    z_s,
    z_r,
    f_sem,
):
    nc = n // 2
    na = nc // 2
    me = lax.axis_index("expert")
    c = lax.rem(me, 2)
    chip = lax.div(me, 2)
    b = lax.rem(chip, 2)
    a = lax.div(chip, 2)
    slot = b * na + a
    oc = 1 - c
    steps, rows_dev, width = tokens_ref.shape
    half = width // 2
    rows = steps * rows_dev
    pair = 2 * rows
    total_rows = nc * pair
    y_rows = na * pair
    units = down.shape[0]
    s_units = sh_part.shape[2]
    fb = shared_down.shape[1]

    def dev(a_at, b_at, c_at):
        return {"expert": (2 * a_at + b_at) * 2 + c_at}

    partner = dev(a, b, oc)
    across = dev(a, 1 - b, c)

    def rcopy(src, dst, send, recv, to):
        return pltpu.make_async_remote_copy(
            src_ref=src,
            dst_ref=dst,
            send_sem=send,
            recv_sem=recv,
            device_id=to,
            device_id_type=pl.DeviceIdType.MESH,
        )

    def a_of(d):
        return lax.rem(a + d, na)

    def a_from(d):
        return lax.rem(a + na - d, na)

    def block(at):
        return pl.ds(pl.multiple_of(at * pair, pair), pair)

    up_rows = width // 8
    loads = []
    offset = lax.rem(me, nc) * fb
    start = pl.multiple_of(lax.div(offset, LANES) * LANES, LANES)
    inner = pl.multiple_of(offset - start, 16)
    loads.append(
        pltpu.make_async_copy(
            shared_up_hbm.at[0], shared_up.at[pl.ds(inner, fb)], w_sem.at[0]
        )
    )
    loads.append(pltpu.make_async_copy(shared_down_hbm.at[0], shared_down, w_sem.at[1]))
    for at in range(8):
        piece = pl.ds(at * up_rows, up_rows)
        loads.append(
            pltpu.make_async_copy(
                gate_up_hbm.at[0, 0, piece], gate_up.at[piece], w_sem.at[2 + at]
            )
        )
    down_rows = units // 4
    for at in range(4):
        piece = pl.ds(at * down_rows, down_rows)
        loads.append(
            pltpu.make_async_copy(down_hbm.at[0, 0, piece], down.at[piece], w_sem.at[10 + at])
        )
    shared_up[...] = jnp.zeros_like(shared_up)

    barrier = pltpu.get_barrier_semaphore()

    def greet(to):
        pl.semaphore_signal(barrier, inc=1, device_id=to, device_id_type=pl.DeviceIdType.MESH)

    greet(partner)
    for d in range(1, nc):
        other = lax.rem(chip + d, nc)
        greet({"expert": other * 2 + c})
    for load in loads:
        load.start()

    lane = lax.broadcasted_iota(jnp.int32, (rows_dev, LANES), 1)
    row_at = lax.broadcasted_iota(jnp.int32, (rows_dev, LANES), 0)
    of_lane = lane & (experts - 1)
    level = lax.div(lane, experts)
    gain = gain_ref[...]
    for step in range(steps):
        h = tokens_ref[step].astype(F32)
        scaling = lax.rsqrt(jnp.mean(h * h, axis=-1, keepdims=True) + EPSILON)
        normed = (h * scaling * gain).astype(BF16).astype(F32)
        ids = ids_ref[0, step]
        gates = gates_ref[0, step]
        dense = jnp.zeros((rows_dev, LANES), F32)
        for k in range(ids.shape[1]):
            dense = dense + jnp.where(ids[:, k : k + 1] == of_lane, gates[:, k : k + 1], 0.0)
        dense = jnp.where(row_at < live_ref[step : step + 1, :], dense, 0.0)
        high = dense.astype(BF16).astype(F32)
        rest = dense - high
        mid = rest.astype(BF16).astype(F32)
        low = rest - mid
        coded = jnp.where(
            level == 0, high, jnp.where(level == 1, mid, jnp.where(level == 2, low, 0.0))
        )
        at = slice(step * rows_dev, (step + 1) * rows_dev)
        for side in range(2):
            own_n[side, at, :half] = normed[:, side * half : (side + 1) * half]
            own_n[side, at, half:] = coded

    pl.semaphore_wait(barrier, nc)

    swap = rcopy(own_n.at[oc], peer_n, n_sem.at[0], n_sem.at[1], partner)
    swap.start()
    swap.wait()
    mine = own_n[c]
    theirs = peer_n[...]
    first = jnp.where(c == 0, mine, theirs)
    second = jnp.where(c == 0, theirs, mine)
    x_all[c, block(slot)] = jnp.concatenate([first, second], axis=0).astype(BF16)

    def gather(buf, zs, ys, ps, rs):
        sent = []

        def push(at, send, to):
            copy = rcopy(buf.at[c, block(at)], buf.at[c, block(at)], send, rs.at[c, at], to)
            copy.start()
            sent.append(copy)

        def arrived(side, at):
            view = buf.at[side, block(at)]
            rcopy(view, view, ps.at[0], rs.at[side, at], partner).wait_recv()

        def begin():
            for d in range(1, na):
                push(slot, zs.at[d], dev(a_of(d), b, c))
            push(slot, ys.at[0], across)
            push(slot, ps.at[0], partner)

        def forward():
            for d in range(1, na):
                at = b * na + a_from(d)
                arrived(c, at)
                push(at, ys.at[d], across)
                push(at, ps.at[d], partner)

        def finish():
            for d in range(na):
                at = (1 - b) * na + a_from(d)
                arrived(c, at)
                push(at, ps.at[na + d], partner)
            for at in range(nc):
                arrived(oc, at)

        return begin, forward, finish, sent

    begin, forward, finish, sent = gather(x_all, xz_s, xy_s, xp_s, x_r)
    begin()
    forward()
    finish()
    pending = list(sent)

    expert = lax.div(me, group)
    codes = x_all[0, :, half:].astype(F32)
    wide = lax.broadcasted_iota(jnp.int32, (total_rows, LANES), 1) & (experts - 1)
    weight = jnp.sum(jnp.where(wide == expert, codes, 0.0), axis=1, keepdims=True)

    s_half = s_units // 2

    def shared_project():
        loads[0].wait()
        features = x_all[lax.div(me, nc), :, pl.ds(start, window)]
        for side in range(2):
            for kind in range(2):
                cols = slice(kind * s_units + side * s_half, kind * s_units + (side + 1) * s_half)
                sh_part[side, :, kind * s_half : (kind + 1) * s_half] = dotted(
                    features, shared_up[:, cols]
                )
        sh_send[...] = sh_part[oc].astype(BF16)
        copy = rcopy(sh_send, sh_peer, sp_sem.at[0], sp_sem.at[1], partner)
        copy.start()
        return copy

    y_own = pl.ds(pl.multiple_of(b * y_rows, y_rows), y_rows)
    y_other = pl.ds(pl.multiple_of((1 - b) * y_rows, y_rows), y_rows)

    def shared_across(copy):
        copy.wait()
        sh_y[...] = (sh_part[c, y_other] + sh_peer[y_other].astype(F32)).astype(BF16)
        out = rcopy(sh_y, sh_yr, sy_sem.at[0], sy_sem.at[1], across)
        out.start()
        return out

    def shared_along(copy):
        copy.wait()
        summed = sh_part[c, y_own] + sh_peer[y_own].astype(F32) + sh_yr[...].astype(F32)
        sh_part[0, :y_rows] = summed
        sh_z[...] = summed.astype(BF16).reshape(na, pair, s_units)
        copies = []
        for d in range(1, na):
            copy = rcopy(
                sh_z.at[a_of(d)],
                sh_zr.at[d],
                sz_s.at[d],
                sz_r.at[d],
                dev(a_of(d), b, c),
            )
            copy.start()
            copies.append(copy)
        return copies

    h_begin, h_forward, h_finish, h_sent = gather(sh_hidden, hz_s, hy_s, hp_s, h_r)

    def shared_active(copies):
        total = sh_part[0, block(a)]
        for d in range(1, na):
            copies[d - 1].wait()
            total = total + sh_zr[d].astype(F32)
        sh_hidden[c, block(slot)] = (
            jax.nn.silu(total[:, :s_half]) * total[:, s_half:]
        ).astype(BF16)
        h_begin()

    def shared_last():
        h_finish()
        pending.extend(h_sent)
        loads[1].wait()
        cols = dotted(sh_hidden[0], shared_down[:s_half]) + dotted(
            sh_hidden[1], shared_down[s_half:]
        )
        so_send[...] = cols.astype(BF16).reshape(nc, pair, fb)
        copies = []
        for d in range(1, nc):
            other = lax.rem(chip + d, nc)
            to_slot = lax.rem(other, 2) * na + lax.div(other, 2)
            copy = rcopy(
                so_send.at[to_slot],
                so_recv.at[chip],
                so_s.at[d],
                so_r.at[chip],
                {"expert": other * 2 + c},
            )
            copy.start()
            copies.append(copy)
        return copies

    def shared_collect(copies):
        for d in range(1, nc):
            other = lax.rem(chip + nc - d, nc)
            view = so_recv.at[other]
            rcopy(view, view, so_s.at[0], so_r.at[other], partner).wait_recv()
        so_recv[chip] = so_send[slot]
        for at in range(nc):
            value = so_recv[at].astype(F32)
            so_f[0, at] = value[:rows]
            so_f[1, at] = value[rows:]
        copy = rcopy(so_f.at[oc], so_fr, f_sem.at[2], f_sem.at[3], partner)
        copy.start()
        for copy_at in copies:
            copy_at.wait_send()
        return copy

    def gate_up_tile(at, tile):
        def product(first_col):
            cols = slice(first_col, first_col + tile)
            return dotted(x_all[0, :, :half], gate_up[:half, cols]) + dotted(
                x_all[1, :, :half], gate_up[half:, cols]
            )

        gate = product(at * tile)
        up = product(units + at * tile)
        hidden[:, at * tile : (at + 1) * tile] = (jax.nn.silu(gate) * up).astype(BF16)

    state = [shared_project()]
    for load in loads[2:10]:
        load.wait()
    tile = min(256, units)
    stages = [
        lambda: state.append(shared_across(state[-1])),
        lambda: state.append(shared_along(state[-1])),
        lambda: shared_active(state[-1]),
        lambda: h_forward(),
    ]
    for at in range(units // tile):
        gate_up_tile(at, tile)
        if stages:
            stages.pop(0)()
    for stage in stages:
        stage()
    for load in loads[10:]:
        load.wait()

    chunks = half // chunk

    def product(side, j):
        cols = pl.ds(pl.multiple_of(side * half + j * chunk, LANES), chunk)
        return dotted(hidden[...], down[:, cols]) * weight

    to_partner = []
    for j in range(chunks):
        r_p[j] = product(oc, j).astype(BF16)
        copy = rcopy(r_p.at[j], r_pr.at[j], p_s.at[j], p_r.at[j], partner)
        copy.start()
        to_partner.append(copy)
    so_copies = shared_last()

    to_across = []
    to_along = []

    def send_across(j):
        part[...] = product(c, j)
        to_partner[j].wait()
        r_y[j] = (part[y_other] + r_pr[j, y_other].astype(F32)).astype(BF16)
        copy = rcopy(r_y.at[j], r_yr.at[j], y_s.at[j], y_r.at[j], across)
        copy.start()
        to_across.append(copy)
        keep[j] = part[y_own] + r_pr[j, y_own].astype(F32)

    def send_along(j):
        to_across[j].wait()
        summed = keep[j] + r_yr[j].astype(F32)
        r_z[j] = summed.astype(BF16).reshape(na, pair, chunk)
        copies = []
        for d in range(1, na):
            copy = rcopy(
                r_z.at[j, a_of(d)],
                r_zr.at[j, d],
                z_s.at[j, d],
                z_r.at[j, d],
                dev(a_of(d), b, c),
            )
            copy.start()
            copies.append(copy)
        to_along.append(copies)
        keep[j] = summed

    def collect(j):
        total = keep[j, block(a)]
        for d in range(1, na):
            to_along[j][d - 1].wait()
            total = total + r_zr[j, d].astype(F32)
        cols = slice(j * chunk, (j + 1) * chunk)
        res[0, :, cols] = total[:rows]
        res[1, :, cols] = total[rows:]

    for j in range(chunks):
        send_across(j)
        if j >= 2:
            send_along(j - 2)
    for j in range(max(chunks - 2, 0), chunks):
        send_along(j)
    shared_swap = shared_collect(so_copies)
    for j in range(chunks):
        collect(j)
    last = rcopy(res.at[oc], res_r, f_sem.at[0], f_sem.at[1], partner)
    last.start()
    own_cols = pl.ds(pl.multiple_of(c * half, LANES), half)
    other_cols = pl.ds(pl.multiple_of(oc * half, LANES), half)
    routed_out[:, own_cols] = res[c]
    shared_swap.wait()
    shared_out[c] = so_f[c]
    shared_out[oc] = so_fr[...]
    last.wait()
    routed_out[:, other_cols] = res_r[...]
    for copy in pending:
        copy.wait_send()


def per_device(
    tokens,
    live_rows,
    expert_ids,
    gate_weights,
    norm_gain,
    expert_gate_up,
    expert_down,
    shared_gate_up,
    shared_down,
):
    step_count, row_count, model_width = tokens.shape
    n = lax.axis_size("expert")
    group = n // EXPERTS
    units = expert_down.shape[2]
    fb, s_wide = shared_gate_up.shape[1:]
    s_units = s_wide // 2
    nc = n // 2
    na = nc // 2
    half = model_width // 2
    rows = step_count * row_count
    pair = 2 * rows
    total = nc * pair
    y_rows = na * pair
    wide = half + LANES
    chunk = next(size for size in (512, 256, 128) if half % size == 0)
    chunks = half // chunk
    span = next(size for size in (128, 64, 32, 16) if fb % size == 0)
    window = -(-(fb + LANES - span) // LANES) * LANES
    dma = pltpu.SemaphoreType.DMA
    vmem = pltpu.VMEM
    whole = pl.BlockSpec(memory_space=pltpu.VMEM)
    anywhere = pl.BlockSpec(memory_space=pl.ANY)
    routed, shared = pl.pallas_call(
        functools.partial(layer_kernel, n, EXPERTS, group, chunk, window),
        out_shape=(
            jax.ShapeDtypeStruct((rows, model_width), F32),
            jax.ShapeDtypeStruct((2, nc, rows, fb), F32),
        ),
        in_specs=[whole] * 5 + [anywhere] * 4,
        out_specs=(whole, whole),
        scratch_shapes=[
            vmem((2, rows, wide), F32),
            vmem((rows, wide), F32),
            vmem((2, total, wide), BF16),
            vmem((model_width, 2 * units), BF16),
            vmem((units, model_width), BF16),
            vmem((window, s_wide), BF16),
            vmem((s_units, fb), BF16),
            vmem((total, units), BF16),
            vmem((2, total, s_units), F32),
            vmem((total, s_units), BF16),
            vmem((total, s_units), BF16),
            vmem((y_rows, s_units), BF16),
            vmem((y_rows, s_units), BF16),
            vmem((na, pair, s_units), BF16),
            vmem((na, pair, s_units), BF16),
            vmem((2, total, s_units // 2), BF16),
            vmem((nc, pair, fb), BF16),
            vmem((nc, pair, fb), BF16),
            vmem((2, nc, rows, fb), F32),
            vmem((nc, rows, fb), F32),
            vmem((total, chunk), F32),
            vmem((chunks, total, chunk), BF16),
            vmem((chunks, total, chunk), BF16),
            vmem((chunks, y_rows, chunk), BF16),
            vmem((chunks, y_rows, chunk), BF16),
            vmem((chunks, na, pair, chunk), BF16),
            vmem((chunks, na, pair, chunk), BF16),
            vmem((chunks, y_rows, chunk), F32),
            vmem((2, rows, half), F32),
            vmem((rows, half), F32),
            dma((14,)),
            dma((2,)),
            dma((na,)),
            dma((na,)),
            dma((nc,)),
            dma((2, nc)),
            dma((na,)),
            dma((na,)),
            dma((nc,)),
            dma((2, nc)),
            dma((2,)),
            dma((2,)),
            dma((na,)),
            dma((na,)),
            dma((nc,)),
            dma((nc,)),
            dma((chunks,)),
            dma((chunks,)),
            dma((chunks,)),
            dma((chunks,)),
            dma((chunks, na)),
            dma((chunks, na)),
            dma((4,)),
        ],
        compiler_params=pltpu.CompilerParams(
            collective_id=0, has_side_effects=True, vmem_limit_bytes=67_043_328
        ),
    )(
        tokens,
        live_rows,
        expert_ids,
        gate_weights,
        norm_gain,
        expert_gate_up,
        expert_down,
        shared_gate_up,
        shared_down,
    )
    shared = jnp.transpose(shared, (2, 1, 0, 3)).reshape(step_count, row_count, model_width)
    routed = routed.reshape(step_count, row_count, model_width)
    live = jnp.arange(row_count, dtype=jnp.int32)[None, :] < live_rows
    update = jnp.where(live[:, :, None], routed + shared, 0.0)
    return (tokens.astype(F32) + update).astype(BF16)


def solution(mesh):
    placed = (
        P(None, ("parts", "expert"), None),
        P(None, ("parts", "expert")),
        P(None, None, ("parts", "expert"), None),
        P(None, None, ("parts", "expert"), None),
        P(),
        P(None, "expert", None, None),
        P(None, "expert", None, None),
        P(None, "expert", None),
        P(None, None, "expert"),
    )
    return jax.shard_map(
        per_device,
        mesh=mesh,
        in_specs=placed,
        out_specs=P(None, ("parts", "expert"), None),
        check_vma=False,
    )
```

```python
import functools

import jax
import jax.numpy as jnp
from jax import lax
from jax.experimental import pallas as pl
from jax.experimental.pallas import tpu as pltpu
from jax.sharding import PartitionSpec as P

EXPERTS = 16
EPSILON = 1e-06
LANES = 128
BF16 = jnp.bfloat16
F32 = jnp.float32


def dotted(left, right):
    return jnp.dot(left, right, preferred_element_type=F32)


def dotted_nt(left, right):
    return lax.dot_general(left, right, (((1,), (1,)), ((), ())), preferred_element_type=F32)


def layer_kernel(
    n,
    experts,
    group,
    chunk,
    window,
    tokens_ref,
    live_ref,
    ids_ref,
    gates_ref,
    gain_ref,
    gate_up_hbm,
    down_hbm,
    shared_up_hbm,
    shared_down_hbm,
    update_out,
    acc,
    own_n,
    peer_n,
    x_all,
    gate_up,
    down,
    shared_up,
    shared_down,
    hidden,
    sh_part,
    sh_send,
    sh_peer,
    sh_y,
    sh_yr,
    sh_z,
    sh_zr,
    sh_hidden,
    so_send,
    so_recv,
    so_f,
    so_fr,
    part,
    r_p,
    r_pr,
    r_y,
    r_yr,
    r_z,
    r_zr,
    keep,
    res,
    res_r,
    w_sem,
    n_sem,
    xz_s,
    xy_s,
    xp_s,
    x_r,
    hz_s,
    hy_s,
    hp_s,
    h_r,
    sp_sem,
    sy_sem,
    sz_s,
    sz_r,
    so_s,
    so_r,
    p_s,
    p_r,
    y_s,
    y_r,
    z_s,
    z_r,
    f_sem,
):
    nc = n // 2
    na = nc // 2
    me = lax.axis_index("expert")
    c = lax.rem(me, 2)
    chip = lax.div(me, 2)
    b = lax.rem(chip, 2)
    a = lax.div(chip, 2)
    slot = b * na + a
    oc = 1 - c
    steps, rows_dev, width = tokens_ref.shape
    half = width // 2
    rows = steps * rows_dev
    pair = 2 * rows
    total_rows = nc * pair
    y_rows = na * pair
    units = down.shape[0]
    s_units = sh_part.shape[2]
    fb = shared_down.shape[0]

    def dev(a_at, b_at, c_at):
        return {"expert": (2 * a_at + b_at) * 2 + c_at}

    partner = dev(a, b, oc)
    across = dev(a, 1 - b, c)

    def rcopy(src, dst, send, recv, to):
        return pltpu.make_async_remote_copy(
            src_ref=src,
            dst_ref=dst,
            send_sem=send,
            recv_sem=recv,
            device_id=to,
            device_id_type=pl.DeviceIdType.MESH,
        )

    def a_of(d):
        return lax.rem(a + d, na)

    def a_from(d):
        return lax.rem(a + na - d, na)

    def block(at):
        return pl.ds(pl.multiple_of(at * pair, pair), pair)

    up_rows = width // 8
    loads = []
    offset = lax.rem(me, nc) * fb
    start = pl.multiple_of(lax.div(offset, LANES) * LANES, LANES)
    inner = pl.multiple_of(offset - start, 16)
    loads.append(
        pltpu.make_async_copy(
            shared_up_hbm.at[0], shared_up.at[pl.ds(inner, fb)], w_sem.at[0]
        )
    )
    loads.append(pltpu.make_async_copy(shared_down_hbm.at[0], shared_down, w_sem.at[1]))
    for at in range(8):
        piece = pl.ds(at * up_rows, up_rows)
        loads.append(
            pltpu.make_async_copy(
                gate_up_hbm.at[0, 0, piece], gate_up.at[piece], w_sem.at[2 + at]
            )
        )
    down_rows = units // 4
    for at in range(4):
        piece = pl.ds(at * down_rows, down_rows)
        loads.append(
            pltpu.make_async_copy(down_hbm.at[0, 0, piece], down.at[piece], w_sem.at[10 + at])
        )
    shared_up[...] = jnp.zeros_like(shared_up)

    barrier = pltpu.get_barrier_semaphore()

    def greet(to):
        pl.semaphore_signal(barrier, inc=1, device_id=to, device_id_type=pl.DeviceIdType.MESH)

    greet(partner)
    for d in range(1, nc):
        other = lax.rem(chip + d, nc)
        greet({"expert": other * 2 + c})
    for load in loads:
        load.start()

    lane = lax.broadcasted_iota(jnp.int32, (rows_dev, LANES), 1)
    row_at = lax.broadcasted_iota(jnp.int32, (rows_dev, LANES), 0)
    of_lane = lane & (experts - 1)
    level = lax.div(lane, experts)
    gain = gain_ref[...]
    for step in range(steps):
        h = tokens_ref[step].astype(F32)
        scaling = lax.rsqrt(jnp.mean(h * h, axis=-1, keepdims=True) + EPSILON)
        normed = (h * scaling * gain).astype(BF16).astype(F32)
        ids = ids_ref[0, step]
        gates = gates_ref[0, step]
        dense = jnp.zeros((rows_dev, LANES), F32)
        for k in range(ids.shape[1]):
            dense = dense + jnp.where(ids[:, k : k + 1] == of_lane, gates[:, k : k + 1], 0.0)
        dense = jnp.where(row_at < live_ref[:, step : step + 1], dense, 0.0)
        high = dense.astype(BF16).astype(F32)
        rest = dense - high
        mid = rest.astype(BF16).astype(F32)
        low = rest - mid
        coded = jnp.where(
            level == 0, high, jnp.where(level == 1, mid, jnp.where(level == 2, low, 0.0))
        )
        at = slice(step * rows_dev, (step + 1) * rows_dev)
        for side in range(2):
            own_n[side, at, :half] = normed[:, side * half : (side + 1) * half]
            own_n[side, at, half:] = coded

    pl.semaphore_wait(barrier, nc)

    swap = rcopy(own_n.at[oc], peer_n, n_sem.at[0], n_sem.at[1], partner)
    swap.start()
    swap.wait()
    mine = own_n[c]
    theirs = peer_n[...]
    first = jnp.where(c == 0, mine, theirs)
    second = jnp.where(c == 0, theirs, mine)
    x_all[c, block(slot)] = jnp.concatenate([first, second], axis=0).astype(BF16)

    def gather(buf, zs, ys, ps, rs):
        sent = []

        def push(at, send, to):
            copy = rcopy(buf.at[c, block(at)], buf.at[c, block(at)], send, rs.at[c, at], to)
            copy.start()
            sent.append(copy)

        def arrived(side, at):
            view = buf.at[side, block(at)]
            rcopy(view, view, ps.at[0], rs.at[side, at], partner).wait_recv()

        def begin():
            for d in range(1, na):
                push(slot, zs.at[d], dev(a_of(d), b, c))
            push(slot, ys.at[0], across)
            push(slot, ps.at[0], partner)

        def forward():
            for d in range(1, na):
                at = b * na + a_from(d)
                arrived(c, at)
                push(at, ys.at[d], across)
                push(at, ps.at[d], partner)

        def finish():
            for d in range(na):
                at = (1 - b) * na + a_from(d)
                arrived(c, at)
                push(at, ps.at[na + d], partner)
            for at in range(nc):
                arrived(oc, at)

        return begin, forward, finish, sent

    begin, forward, finish, sent = gather(x_all, xz_s, xy_s, xp_s, x_r)
    begin()
    forward()
    finish()
    pending = list(sent)

    expert = lax.div(me, group)
    codes = x_all[0, :, half:].astype(F32)
    wide = lax.broadcasted_iota(jnp.int32, (total_rows, LANES), 1) & (experts - 1)
    weight = jnp.sum(jnp.where(wide == expert, codes, 0.0), axis=1, keepdims=True)

    s_half = s_units // 2

    def shared_project():
        loads[0].wait()
        features = x_all[lax.div(me, nc), :, pl.ds(start, window)]
        for side in range(2):
            for kind in range(2):
                cols = slice(kind * s_units + side * s_half, kind * s_units + (side + 1) * s_half)
                sh_part[side, :, kind * s_half : (kind + 1) * s_half] = dotted(
                    features, shared_up[:, cols]
                )
        sh_send[...] = sh_part[oc].astype(BF16)
        copy = rcopy(sh_send, sh_peer, sp_sem.at[0], sp_sem.at[1], partner)
        copy.start()
        return copy

    y_own = pl.ds(pl.multiple_of(b * y_rows, y_rows), y_rows)
    y_other = pl.ds(pl.multiple_of((1 - b) * y_rows, y_rows), y_rows)

    def shared_across(copy):
        copy.wait()
        sh_y[...] = (sh_part[c, y_other] + sh_peer[y_other].astype(F32)).astype(BF16)
        out = rcopy(sh_y, sh_yr, sy_sem.at[0], sy_sem.at[1], across)
        out.start()
        return out

    def shared_along(copy):
        copy.wait()
        summed = sh_part[c, y_own] + sh_peer[y_own].astype(F32) + sh_yr[...].astype(F32)
        sh_part[0, :y_rows] = summed
        sh_z[...] = summed.astype(BF16).reshape(na, pair, s_units)
        copies = []
        for d in range(1, na):
            copy = rcopy(
                sh_z.at[a_of(d)],
                sh_zr.at[d],
                sz_s.at[d],
                sz_r.at[d],
                dev(a_of(d), b, c),
            )
            copy.start()
            copies.append(copy)
        return copies

    h_begin, h_forward, h_finish, h_sent = gather(sh_hidden, hz_s, hy_s, hp_s, h_r)

    def shared_active(copies):
        total = sh_part[0, block(a)]
        for d in range(1, na):
            copies[d - 1].wait()
            total = total + sh_zr[d].astype(F32)
        sh_hidden[c, block(slot)] = (
            jax.nn.silu(total[:, :s_half]) * total[:, s_half:]
        ).astype(BF16)
        h_begin()

    def shared_last():
        h_finish()
        pending.extend(h_sent)
        loads[1].wait()
        cols = dotted_nt(sh_hidden[0], shared_down[:, :s_half]) + dotted_nt(
            sh_hidden[1], shared_down[:, s_half:]
        )
        so_send[...] = cols.astype(BF16).reshape(nc, pair, fb)
        copies = []
        for d in range(1, nc):
            other = lax.rem(chip + d, nc)
            to_slot = lax.rem(other, 2) * na + lax.div(other, 2)
            copy = rcopy(
                so_send.at[to_slot],
                so_recv.at[chip],
                so_s.at[d],
                so_r.at[chip],
                {"expert": other * 2 + c},
            )
            copy.start()
            copies.append(copy)
        return copies

    def shared_collect(copies):
        for d in range(1, nc):
            other = lax.rem(chip + nc - d, nc)
            view = so_recv.at[other]
            rcopy(view, view, so_s.at[0], so_r.at[other], partner).wait_recv()
        so_recv[chip] = so_send[slot]
        for at in range(nc):
            value = so_recv[at].astype(F32)
            so_f[0, at] = value[:rows]
            so_f[1, at] = value[rows:]
        copy = rcopy(so_f.at[oc], so_fr, f_sem.at[2], f_sem.at[3], partner)
        copy.start()
        for copy_at in copies:
            copy_at.wait_send()
        return copy

    def gate_up_tile(at, tile):
        def product(first_col):
            cols = slice(first_col, first_col + tile)
            return dotted(x_all[0, :, :half], gate_up[:half, cols]) + dotted(
                x_all[1, :, :half], gate_up[half:, cols]
            )

        gate = product(at * tile)
        up = product(units + at * tile)
        hidden[:, at * tile : (at + 1) * tile] = (jax.nn.silu(gate) * up).astype(BF16)

    state = [shared_project()]
    for load in loads[2:10]:
        load.wait()
    tile = min(256, units)
    for at in range(units // tile):
        gate_up_tile(at, tile)
        if at == 0:
            state.append(shared_across(state[-1]))
    for load in loads[10:]:
        load.wait()

    chunks = half // chunk

    def product(side, j):
        cols = pl.ds(pl.multiple_of(side * half + j * chunk, LANES), chunk)
        return dotted(hidden[...], down[:, cols]) * weight

    to_partner = []

    def send_partner(j):
        r_p[j] = product(oc, j).astype(BF16)
        copy = rcopy(r_p.at[j], r_pr.at[j], p_s.at[j], p_r.at[j], partner)
        copy.start()
        to_partner.append(copy)

    to_across = []
    to_along = []

    def send_across(j):
        part[...] = product(c, j)
        to_partner[j].wait()
        r_y[j] = (part[y_other] + r_pr[j, y_other].astype(F32)).astype(BF16)
        copy = rcopy(r_y.at[j], r_yr.at[j], y_s.at[j], y_r.at[j], across)
        copy.start()
        to_across.append(copy)
        keep[j] = part[y_own] + r_pr[j, y_own].astype(F32)

    def send_along(j):
        to_across[j].wait()
        summed = keep[j] + r_yr[j].astype(F32)
        r_z[j] = summed.astype(BF16).reshape(na, pair, chunk)
        copies = []
        for d in range(1, na):
            copy = rcopy(
                r_z.at[j, a_of(d)],
                r_zr.at[j, d],
                z_s.at[j, d],
                z_r.at[j, d],
                dev(a_of(d), b, c),
            )
            copy.start()
            copies.append(copy)
        to_along.append(copies)
        keep[j] = summed

    def collect(j):
        total = keep[j, block(a)]
        for d in range(1, na):
            to_along[j][d - 1].wait()
            total = total + r_zr[j, d].astype(F32)
        cols = slice(j * chunk, (j + 1) * chunk)
        res[0, :, cols] = total[:rows]
        res[1, :, cols] = total[rows:]

    stages = {
        0: lambda: state.append(shared_along(state[-1])),
        2: lambda: shared_active(state[-1]),
        4: h_forward,
        5: lambda: state.append(shared_last()),
    }
    for j in range(min(2, chunks)):
        send_partner(j)
    for j in range(max(chunks, 6)):
        if j + 2 < chunks:
            send_partner(j + 2)
        if j < chunks:
            send_across(j)
        if 2 <= j and j - 2 < chunks:
            send_along(j - 2)
        if j in stages:
            stages[j]()
    for j in range(max(chunks, 6) - 2, chunks):
        send_along(j)
    so_copies = state[-1]
    shared_swap = shared_collect(so_copies)
    for j in range(chunks):
        collect(j)
    last = rcopy(res.at[oc], res_r, f_sem.at[0], f_sem.at[1], partner)
    last.start()
    own_cols = pl.ds(pl.multiple_of(c * half, LANES), half)
    other_cols = pl.ds(pl.multiple_of(oc * half, LANES), half)
    acc[:, own_cols] = res[c]
    shared_swap.wait()
    last.wait()
    acc[:, other_cols] = res_r[...]
    for at in range(nc):
        slot_chip = so_f[c, at]
        peer_chip = so_fr[at]
        for side in range(2):
            cols = slice((2 * at + side) * fb, (2 * at + side + 1) * fb)
            acc[:, cols] = acc[:, cols] + jnp.where(c == side, slot_chip, peer_chip)
    for step in range(steps):
        update_out[step] = acc[step * rows_dev : (step + 1) * rows_dev]
    for copy in pending:
        copy.wait_send()


def per_device(
    tokens,
    live_rows,
    expert_ids,
    gate_weights,
    norm_gain,
    expert_gate_up,
    expert_down,
    shared_gate_up,
    shared_down,
):
    step_count, row_count, model_width = tokens.shape
    n = lax.axis_size("expert")
    group = n // EXPERTS
    units = expert_down.shape[2]
    fb, s_wide = shared_gate_up.shape[1:]
    s_units = s_wide // 2
    nc = n // 2
    na = nc // 2
    half = model_width // 2
    rows = step_count * row_count
    pair = 2 * rows
    total = nc * pair
    y_rows = na * pair
    wide = half + LANES
    chunk = next(size for size in (512, 256, 128) if half % size == 0)
    chunks = half // chunk
    span = next(size for size in (128, 64, 32, 16) if fb % size == 0)
    window = -(-(fb + LANES - span) // LANES) * LANES
    dma = pltpu.SemaphoreType.DMA
    vmem = pltpu.VMEM
    whole = pl.BlockSpec(memory_space=pltpu.VMEM)
    anywhere = pl.BlockSpec(memory_space=pl.ANY)
    update = pl.pallas_call(
        functools.partial(layer_kernel, n, EXPERTS, group, chunk, window),
        out_shape=jax.ShapeDtypeStruct(tokens.shape, F32),
        in_specs=[whole] * 5 + [anywhere] * 4,
        out_specs=whole,
        scratch_shapes=[
            vmem((rows, model_width), F32),
            vmem((2, rows, wide), F32),
            vmem((rows, wide), F32),
            vmem((2, total, wide), BF16),
            vmem((model_width, 2 * units), BF16),
            vmem((units, model_width), BF16),
            vmem((window, s_wide), BF16),
            vmem((fb, s_units), BF16),
            vmem((total, units), BF16),
            vmem((2, total, s_units), F32),
            vmem((total, s_units), BF16),
            vmem((total, s_units), BF16),
            vmem((y_rows, s_units), BF16),
            vmem((y_rows, s_units), BF16),
            vmem((na, pair, s_units), BF16),
            vmem((na, pair, s_units), BF16),
            vmem((2, total, s_units // 2), BF16),
            vmem((nc, pair, fb), BF16),
            vmem((nc, pair, fb), BF16),
            vmem((2, nc, rows, fb), F32),
            vmem((nc, rows, fb), F32),
            vmem((total, chunk), F32),
            vmem((chunks, total, chunk), BF16),
            vmem((chunks, total, chunk), BF16),
            vmem((chunks, y_rows, chunk), BF16),
            vmem((chunks, y_rows, chunk), BF16),
            vmem((chunks, na, pair, chunk), BF16),
            vmem((chunks, na, pair, chunk), BF16),
            vmem((chunks, y_rows, chunk), F32),
            vmem((2, rows, half), F32),
            vmem((rows, half), F32),
            dma((14,)),
            dma((2,)),
            dma((na,)),
            dma((na,)),
            dma((nc,)),
            dma((2, nc)),
            dma((na,)),
            dma((na,)),
            dma((nc,)),
            dma((2, nc)),
            dma((2,)),
            dma((2,)),
            dma((na,)),
            dma((na,)),
            dma((nc,)),
            dma((nc,)),
            dma((chunks,)),
            dma((chunks,)),
            dma((chunks,)),
            dma((chunks,)),
            dma((chunks, na)),
            dma((chunks, na)),
            dma((4,)),
        ],
        compiler_params=pltpu.CompilerParams(
            collective_id=0, has_side_effects=True, vmem_limit_bytes=67_043_328
        ),
    )(
        tokens,
        live_rows.T,
        expert_ids,
        gate_weights,
        norm_gain,
        expert_gate_up,
        expert_down,
        shared_gate_up,
        jnp.swapaxes(shared_down, 1, 2),
    )
    live = jnp.arange(row_count, dtype=jnp.int32)[None, :] < live_rows
    update = jnp.where(live[:, :, None], update, 0.0)
    return (tokens.astype(F32) + update).astype(BF16)


def solution(mesh):
    placed = (
        P(None, ("parts", "expert"), None),
        P(None, ("parts", "expert")),
        P(None, None, ("parts", "expert"), None),
        P(None, None, ("parts", "expert"), None),
        P(),
        P(None, "expert", None, None),
        P(None, "expert", None, None),
        P(None, "expert", None),
        P(None, None, "expert"),
    )
    return jax.shard_map(
        per_device,
        mesh=mesh,
        in_specs=placed,
        out_specs=P(None, ("parts", "expert"), None),
        check_vma=False,
    )
```
